32 devices in a mesh: groups: 2 (over x), rows: 16 (over z, y, core).
Axes of the slice: x: 2, y: 2, z: 4, core: 2. Of those that a mesh axis runs over, the one named last changes fastest.
Arguments:
- tap_two: bfloat16 [6144, 1024], P(('groups', 'rows')), parts along dimension 0, may hold values from -6 to 6
- coarse_path: bfloat16 [6144, 256], P(('groups', 'rows')), parts along dimension 0, may hold values from -6 to 6
- proj_weight: bfloat16 [1024, 512], replicated, may hold values from -0.1875 to 0.1875
- proj_bias: float32 [512], replicated, may hold values from -3 to 3
- lift_weight: bfloat16 [512, 2048], replicated, may hold values from -0.25 to 0.25
- lift_bias: float32 [512], replicated, may hold values from -3 to 3
- merge_weight: bfloat16 [4608, 256], replicated, may hold values from -0.09375 to 0.09375
- out_weight: bfloat16 [256, 256], replicated, may hold values from -0.375 to 0.375
- out_bias: float32 [256], replicated, may hold values from -3 to 3
- first_inner_w: bfloat16 [2304, 256], replicated, may hold values from -0.125 to 0.125
- first_inner_b: float32 [256], replicated, may hold values from -3 to 3
- first_outer_w: bfloat16 [2304, 256], replicated, may hold values from -0.125 to 0.125
- first_outer_b: float32 [256], replicated, may hold values from -3 to 3
- second_inner_w: bfloat16 [2304, 256], replicated, may hold values from -0.125 to 0.125
- second_inner_b: float32 [256], replicated, may hold values from -3 to 3
- second_outer_w: bfloat16 [2304, 256], replicated, may hold values from -0.125 to 0.125
- second_outer_b: float32 [256], replicated, may hold values from -3 to 3
Outputs:
- united: bfloat16 [64, 384, 256], P(('groups', 'rows')), parts along dimension 0
The draws below stay inside these ranges and needn't reach their ends.
There are 2 independent parts, one for each index of `groups`. The reference program is written for one: setup_inputs(seed, part) draws one part's arguments, and reference() takes and returns one part's arrays. A program takes and returns all parts, laid end to end along the dimension named above; an argument that names none is the same for every part. Nothing has to cross between parts.
All inputs are finite; a program needn't handle non-finite values.
Results may differ from the reference program's by a relative error of at most 0.0075.
Values may be sent and summed in bfloat16 or wider, within the bound.
A program may use at most 64 MiB of HBM per device.

```python
import jax
import jax.numpy as jnp

D = 1024
FEAT2 = 512
F = 256
GW = 192
GH = 16
TOKENS = 3072


def shard_levels(own_key, dims, pieces, least, top_value):
    gain, own = 1.0, jax.random.fold_in(own_key, 6)
    for dim, shards_of in pieces:
        steps = jnp.exp(jax.random.uniform(jax.random.fold_in(own, dim), (shards_of,), jnp.float32, least / len(pieces), top_value / len(pieces)))
        gain = gain * jnp.repeat(steps, dims[dim] // shards_of).reshape([-1 if axis == dim else 1 for axis in range(len(dims))])
    return gain


def centred(rng, extent, width, bound, cuts=(), dtype=jnp.bfloat16):
    entries = jax.random.normal(rng, extent, jnp.float32) * width
    if len(cuts) > 0:
        entries = shard_levels(rng, extent, cuts, -0.22, 0.18) * entries
    return jnp.clip(entries, min=-bound, max=bound).astype(dtype)


def setup_inputs(seed: int = 0, part: int = 0) -> dict:
    arg_keys = jax.random.split(jax.random.key(seed), 18)
    part_keys = jax.random.split(jax.random.fold_in(arg_keys[17], part), 18)
    return {
        "tap_two": centred(part_keys[0], (TOKENS, D), 1.0, 6.0, ((0, 16),)),
        "coarse_path": centred(part_keys[1], (TOKENS, F), 1.0, 6.0, ((0, 16),)),
        "proj_weight": centred(arg_keys[2], (D, FEAT2), D ** -0.5, 0.1875),
        "proj_bias": centred(arg_keys[3], (FEAT2,), 0.5, 3.0, (), jnp.float32),
        "lift_weight": centred(arg_keys[4], (FEAT2, 4 * FEAT2), FEAT2 ** -0.5, 0.25),
        "lift_bias": centred(arg_keys[5], (FEAT2,), 0.5, 3.0, (), jnp.float32),
        "merge_weight": centred(arg_keys[6], (9 * FEAT2, F), (9 * FEAT2) ** -0.5, 0.09375),
        "out_weight": centred(arg_keys[7], (F, F), F ** -0.5, 0.375),
        "out_bias": centred(arg_keys[8], (F,), 0.5, 3.0, (), jnp.float32),
        "first_inner_w": centred(arg_keys[9], (9 * F, F), (9 * F) ** -0.5, 0.125),
        "first_inner_b": centred(arg_keys[10], (F,), 0.5, 3.0, (), jnp.float32),
        "first_outer_w": centred(arg_keys[11], (9 * F, F), (9 * F) ** -0.5, 0.125),
        "first_outer_b": centred(arg_keys[12], (F,), 0.5, 3.0, (), jnp.float32),
        "second_inner_w": centred(arg_keys[13], (9 * F, F), (9 * F) ** -0.5, 0.125),
        "second_inner_b": centred(arg_keys[14], (F,), 0.5, 3.0, (), jnp.float32),
        "second_outer_w": centred(arg_keys[15], (9 * F, F), (9 * F) ** -0.5, 0.125),
        "second_outer_b": centred(arg_keys[16], (F,), 0.5, 3.0, (), jnp.float32),
    }


def conv_grid(grid, weight):
    height, across, channels = grid.shape
    padded = jnp.pad(grid, ((1, 1), (1, 1), (0, 0)))
    total = jnp.zeros((height * across, weight.shape[1]), jnp.float32)
    for offset_row in range(3):
        for offset_col in range(3):
            tap_index = offset_row * 3 + offset_col
            shifted = padded[offset_row:offset_row + height, offset_col:offset_col + across].reshape(height * across, channels)
            total = total + jnp.dot(shifted, weight[tap_index * channels:(tap_index + 1) * channels], preferred_element_type=jnp.float32)
    return total.reshape(height, across, weight.shape[1])


def enlarge(grown):
    upper = 0.25 * grown[:-2] + 0.75 * grown[1:-1]
    lower = 0.75 * grown[1:-1] + 0.25 * grown[2:]

    def sideways(band):
        return (0.25 * band[:, :-2] + 0.75 * band[:, 1:-1], 0.75 * band[:, 1:-1] + 0.25 * band[:, 2:])

    upper_left, upper_right = sideways(upper)
    lower_left, lower_right = sideways(lower)
    top_pair = jnp.stack([upper_left, upper_right], axis=2)
    bottom_pair = jnp.stack([lower_left, lower_right], axis=2)
    joined = jnp.stack([top_pair, bottom_pair], axis=1)
    height, across, channels = upper_left.shape
    return joined.reshape(2 * height, 2 * across, channels)


def residual_unit(value, inner_w, inner_b, outer_w, outer_b, extra):
    first_pass = conv_grid(jnp.maximum(value, 0), inner_w) + inner_b
    inner = jnp.maximum(first_pass, 0.0).astype(jnp.bfloat16)
    return conv_grid(inner, outer_w) + outer_b + value.astype(jnp.float32) + extra


def reference(tap_two, coarse_path, proj_weight, proj_bias, lift_weight, lift_bias, merge_weight, out_weight, out_bias, first_inner_w, first_inner_b, first_outer_w, first_outer_b, second_inner_w, second_inner_b, second_outer_w, second_outer_b):
    projected = (jnp.dot(tap_two, proj_weight, preferred_element_type=jnp.float32) + proj_bias).astype(jnp.bfloat16)
    lifted = jnp.dot(projected, lift_weight, preferred_element_type=jnp.float32).reshape(GH, GW, 2, 2, FEAT2) + lift_bias
    widened = lifted.transpose(0, 2, 1, 3, 4).reshape(2 * GH, 2 * GW, FEAT2).astype(jnp.bfloat16)
    reassembled = conv_grid(widened, merge_weight).astype(jnp.bfloat16)
    coarse_grid = coarse_path.reshape(GH, GW, F).astype(jnp.float32)
    padded = jnp.pad(coarse_grid, ((1, 1), (1, 1), (0, 0)), mode="edge")
    spread = enlarge(padded).astype(jnp.bfloat16)
    carried = (jnp.dot(spread.reshape(4 * GH * GW, F), out_weight, preferred_element_type=jnp.float32) + out_bias).reshape(2 * GH, 2 * GW, F)
    merged = residual_unit(reassembled, first_inner_w, first_inner_b, first_outer_w, first_outer_b, carried).astype(jnp.bfloat16)
    united = residual_unit(merged, second_inner_w, second_inner_b, second_outer_w, second_outer_b, 0.0).astype(jnp.bfloat16)
    return united
```

```python
import functools

import jax
import jax.numpy as jnp
from jax import lax
from jax.experimental import pallas as pl
from jax.experimental.pallas import tpu as pltpu
from jax.sharding import PartitionSpec as P

GW = 192
BF16 = jnp.bfloat16
F32 = jnp.float32

PJ_SIB, PJ_ONE, PJ_TWO, PJ_THREE, CO_SIB, CO_ONE, CO_TWO, S_REA, S_IN1, S_MER, S_IN2 = range(11)


def dot(a, b):
    return jnp.dot(a, b, preferred_element_type=F32)


def put(slab, row, even, odd):
    width, chans = even.shape
    at = lax.broadcasted_iota(jnp.int32, even.shape, 0)
    before = jnp.where(at == 0, 0.0, pltpu.roll(odd, 1, 0))
    after = jnp.where(at == width - 1, 0.0, pltpu.roll(even, width - 1, 0))
    for group, value in enumerate((before, even, odd, after)):
        slab[row, :, group * chans : (group + 1) * chans] = value.astype(BF16)


def kernel(
    count,
    tap_h,
    coarse_h,
    proj_h,
    proj_bh,
    lift_h,
    lift_bh,
    merge_h,
    out_h,
    out_bh,
    fi_h,
    fi_bh,
    fo_h,
    fo_bh,
    si_h,
    si_bh,
    so_h,
    so_bh,
    result,
    tap,
    coarse,
    proj_w,
    proj_b,
    lift_w,
    lift_b,
    merge_w,
    out_w,
    out_b,
    fi_w,
    fi_b,
    fo_w,
    fo_b,
    si_w,
    si_b,
    so_w,
    so_b,
    pj,
    wid,
    rea,
    rea_raw,
    carried,
    in1,
    mer,
    mer_raw,
    in2,
    local_sem,
    send_sem,
    recv_sem,
):
    width = tap.shape[0]
    feat = proj_w.shape[1]
    chans = out_w.shape[1]
    me = lax.axis_index("rows")
    side = lax.rem(me, 2)
    step = 2 * side - 1
    sibling = me - step

    def inside(device):
        return jnp.logical_and(device >= 0, device < count)

    valid = (True, inside(me + step), inside(me + 2 * step), inside(me + 3 * step))
    back_two = inside(me - 2 * step)

    started = []

    def fetch(src, dst):
        copy = pltpu.make_async_copy(src, dst, local_sem.at[len(started)])
        started.append(copy)
        copy.start()
        return [copy]

    def fetch_conv(src, dst):
        part = src.shape[0] // 3
        copies = []
        for k in range(3):
            where = pl.multiple_of((side * k + (1 - side) * (2 - k)) * part, part)
            copies += fetch(src.at[pl.ds(where, part)], dst.at[pl.ds(k * part, part)])
        return copies

    def done(copies):
        for copy in copies:
            copy.wait()

    coarse_in = fetch(coarse_h, coarse.at[0])
    tap_in = fetch(tap_h, tap) + fetch(proj_h, proj_w) + fetch(proj_bh, proj_b)
    lift_in = fetch(lift_bh, lift_b)
    half = 2 * feat
    for m in range(2):
        where = pl.multiple_of((side * m + (1 - side) * (1 - m)) * half, half)
        lift_in += fetch(lift_h.at[:, pl.ds(where, half)], lift_w.at[:, pl.ds(m * half, half)])

    partners = (
        (me + step, valid[1]),
        (me + 2 * step, valid[2]),
        (me - 2 * step, back_two),
        (me + 3 * step, valid[3]),
    )
    barrier = pltpu.get_barrier_semaphore()
    expected = jnp.int32(1)
    pl.semaphore_signal(
        barrier, inc=1, device_id={"rows": sibling}, device_id_type=pl.DeviceIdType.MESH
    )
    for device, there in partners:

        @pl.when(there)
        def _():
            pl.semaphore_signal(
                barrier, inc=1, device_id={"rows": device}, device_id_type=pl.DeviceIdType.MESH
            )

        expected = expected + there.astype(jnp.int32)
    pl.semaphore_wait(barrier, expected)

    def remote(src, dst, kind, device):
        return pltpu.make_async_remote_copy(
            src_ref=src,
            dst_ref=dst,
            send_sem=send_sem.at[kind],
            recv_sem=recv_sem.at[kind],
            device_id={"rows": device},
            device_id_type=pl.DeviceIdType.MESH,
        )

    sent = []

    def send(src, dst, kind, device, there=None):
        sent.append((remote(src, dst, kind, device), there))
        if there is None:
            sent[-1][0].start()
        else:
            pl.when(there)(sent[-1][0].start)

    def received(dst, kind, there=None):
        copy = remote(dst, dst, kind, sibling)
        if there is None:
            copy.wait_recv()
        else:
            pl.when(there)(copy.wait_recv)

    done(coarse_in)
    send(coarse.at[0], coarse.at[3], CO_SIB, sibling)

    merge_in = fetch_conv(merge_h, merge_w)
    out_in = fetch(out_h, out_w) + fetch(out_bh, out_b)
    fi_in = fetch(fi_bh, fi_b) + fetch_conv(fi_h, fi_w)
    fo_in = fetch(fo_bh, fo_b) + fetch_conv(fo_h, fo_w)
    si_in = fetch(si_bh, si_b) + fetch_conv(si_h, si_w)
    so_in = fetch(so_bh, so_b) + fetch_conv(so_h, so_w)

    done(tap_in)
    pj[0] = (dot(tap[...], proj_w[...]) + proj_b[...]).astype(BF16)
    send(pj.at[0], pj.at[1], PJ_ONE, me + step, valid[1])
    send(pj.at[0], pj.at[4], PJ_SIB, sibling)
    send(pj.at[0], pj.at[3], PJ_THREE, me + 3 * step, valid[3])
    send(coarse.at[0], coarse.at[1], CO_ONE, me + step, valid[1])
    at_end = jnp.logical_and(back_two, jnp.logical_not(valid[1]))
    send(pj.at[0], pj.at[2], PJ_TWO, me - 2 * step, at_end)
    send(coarse.at[0], coarse.at[2], CO_TWO, me - 2 * step, at_end)

    def lift(token, slab_token, halves):
        for m in halves:
            both = dot(pj[slab_token], lift_w[:, m * half : (m + 1) * half])
            even = both[:, :feat] + lift_b[...]
            odd = both[:, feat:] + lift_b[...]
            if token > 0:
                even = jnp.where(valid[token], even, 0.0)
                odd = jnp.where(valid[token], odd, 0.0)
            put(wid, 2 * token + m + 1, even, odd)

    def conv(slab, weight, low, high):
        group = slab.shape[2] // 4
        rows = high - low
        sides = []
        for parity in range(2):
            total = None
            for k in range(3):
                cells = slab[low + k : high + k, :, parity * group : (parity + 3) * group]
                term = dot(
                    cells.reshape(rows * width, 3 * group),
                    weight[k * 3 * group : (k + 1) * 3 * group, :],
                )
                total = term if total is None else total + term
            sides.append(total.reshape(rows, width, chans))
        return sides

    def keep(row, value):
        return value if row < 2 else jnp.where(valid[row // 2], value, 0.0)

    def merge_rows(low, high):
        even, odd = conv(wid, merge_w, low, high)
        for row in range(low, high):
            e, o = keep(row, even[row - low]), keep(row, odd[row - low])
            if row < 4:
                rea_raw[row, :, :chans] = e.astype(BF16)
                rea_raw[row, :, chans:] = o.astype(BF16)
            put(rea, row + 1, jnp.maximum(e, 0.0), jnp.maximum(o, 0.0))

    def inner_rows(src, weight, bias, dst, low, high):
        even, odd = conv(src, weight, low, high)
        for row in range(low, high):
            e = jnp.maximum(even[row - low] + bias[...], 0.0)
            o = jnp.maximum(odd[row - low] + bias[...], 0.0)
            put(dst, row + 1, keep(row, e), keep(row, o))

    def merged_rows(low, high):
        even, odd = conv(in1, fo_w, low, high)
        for row in range(low, high):
            outer = []
            for parity, value in enumerate((even, odd)):
                lanes = slice(parity * chans, (parity + 1) * chans)
                whole = (
                    value[row - low]
                    + fo_b[...]
                    + rea_raw[row, :, lanes].astype(F32)
                    + carried[row, :, lanes]
                )
                whole = keep(row, whole)
                if row < 2:
                    mer_raw[row, :, lanes] = whole.astype(BF16)
                outer.append(jnp.maximum(whole, 0.0))
            put(mer, row + 1, *outer)

    def carry(row, near, far):
        band = 0.75 * coarse[near].astype(F32) + 0.25 * coarse[far].astype(F32)
        at = lax.broadcasted_iota(jnp.int32, band.shape, 0)
        before = jnp.where(at == 0, band, pltpu.roll(band, 1, 0))
        after = jnp.where(at == width - 1, band, pltpu.roll(band, width - 1, 0))
        for parity, other in enumerate((before, after)):
            spread = (0.75 * band + 0.25 * other).astype(BF16)
            carried[row, :, parity * chans : (parity + 1) * chans] = (
                dot(spread, out_w[...]) + out_b[...]
            )

    done(lift_in)
    lift(0, 0, (0, 1))
    received(pj.at[4], PJ_SIB)
    lift(-1, 4, (1,))
    done(merge_in)
    merge_rows(0, 1)
    send(rea.at[1], rea.at[0], S_REA, sibling)

    done(out_in)
    received(coarse.at[3], CO_SIB)
    carry(0, 0, 3)

    @pl.when(jnp.logical_not(valid[1]))
    def _():
        coarse[1] = coarse[0]
        pj[1] = jnp.zeros_like(pj[1])

    received(pj.at[1], PJ_ONE, valid[1])
    send(pj.at[1], pj.at[2], PJ_TWO, me + 3 * step, valid[3])
    lift(1, 1, (0, 1))
    received(coarse.at[1], CO_ONE, valid[1])
    send(coarse.at[1], coarse.at[2], CO_TWO, me + 3 * step, valid[3])
    merge_rows(1, 3)
    received(rea.at[0], S_REA)
    done(fi_in)
    inner_rows(rea, fi_w, fi_b, in1, 0, 1)
    send(in1.at[1], in1.at[0], S_IN1, sibling)
    inner_rows(rea, fi_w, fi_b, in1, 1, 2)
    done(fo_in)
    received(in1.at[0], S_IN1)
    merged_rows(0, 1)
    send(mer.at[1], mer.at[0], S_MER, sibling)

    @pl.when(jnp.logical_not(valid[2]))
    def _():
        pj[2] = jnp.zeros_like(pj[2])

    @pl.when(jnp.logical_not(valid[3]))
    def _():
        pj[3] = jnp.zeros_like(pj[3])

    carry(1, 0, 1)
    carry(2, 1, 0)
    received(pj.at[2], PJ_TWO, valid[2])
    lift(2, 2, (0, 1))
    received(pj.at[3], PJ_THREE, valid[3])
    lift(3, 3, (0,))
    merge_rows(3, 6)
    inner_rows(rea, fi_w, fi_b, in1, 2, 5)

    @pl.when(jnp.logical_not(valid[2]))
    def _():
        coarse[2] = coarse[1]

    received(coarse.at[2], CO_TWO, valid[2])
    carry(3, 1, 2)
    merged_rows(1, 4)
    done(si_in)
    received(mer.at[0], S_MER)
    inner_rows(mer, si_w, si_b, in2, 0, 1)
    send(in2.at[1], in2.at[0], S_IN2, sibling)
    inner_rows(mer, si_w, si_b, in2, 1, 3)
    done(so_in)

    line = lax.broadcasted_iota(jnp.int32, (2 * width, 2 * width), 0)
    column = lax.broadcasted_iota(jnp.int32, (2 * width, 2 * width), 1)
    weave = (column == line // 2 + width * (line % 2)).astype(F32).astype(BF16)
    for row in (1, 0):
        if row == 0:
            received(in2.at[0], S_IN2)
        sides = conv(in2, so_w, row, row + 1)
        united = [
            (sides[parity][0] + so_b[...] + mer_raw[row, :, parity * chans : (parity + 1) * chans].astype(F32)).astype(BF16)
            for parity in range(2)
        ]
        woven = dot(weave, jnp.concatenate(united, axis=0)).astype(BF16)
        target = side * row + (1 - side) * (1 - row)
        result[pl.ds(target, 1)] = woven[None]

    for copy, there in sent:
        if there is None:
            copy.wait_send()
        else:
            pl.when(there)(copy.wait_send)


def body(*args):
    count = lax.axis_size("rows")
    tap_two, coarse_path, proj_weight = args[:3]
    tokens, depth = tap_two.shape
    feat, chans = proj_weight.shape[1], coarse_path.shape[1]
    assert tokens == GW and count % 2 == 0
    args = [arg.reshape(1, -1) if arg.ndim == 1 else arg for arg in args]

    scratch = []
    for place, arg in enumerate(args):
        shape = (4, *arg.shape) if place == 1 else arg.shape
        scratch.append(pltpu.VMEM(shape, arg.dtype))
    scratch += [
        pltpu.VMEM((5, tokens, feat), BF16),
        pltpu.VMEM((8, tokens, 4 * feat), BF16),
        pltpu.VMEM((7, tokens, 4 * chans), BF16),
        pltpu.VMEM((4, tokens, 2 * chans), BF16),
        pltpu.VMEM((4, tokens, 2 * chans), F32),
        pltpu.VMEM((6, tokens, 4 * chans), BF16),
        pltpu.VMEM((5, tokens, 4 * chans), BF16),
        pltpu.VMEM((2, tokens, 2 * chans), BF16),
        pltpu.VMEM((4, tokens, 4 * chans), BF16),
        pltpu.SemaphoreType.DMA((28,)),
        pltpu.SemaphoreType.DMA((11,)),
        pltpu.SemaphoreType.DMA((11,)),
    ]
    mid = pl.pallas_call(
        functools.partial(kernel, count),
        out_shape=pltpu.VMEM((2, 2 * tokens, chans), BF16),
        in_specs=[pl.BlockSpec(memory_space=pl.ANY)] * len(args),
        out_specs=pl.BlockSpec(memory_space=pltpu.VMEM),
        scratch_shapes=scratch,
        compiler_params=pltpu.CompilerParams(
            collective_id=0, has_side_effects=True, vmem_limit_bytes=60 * 2**20
        ),
        name="fused_tap",
    )(*args)

    return mid


def solution(mesh):
    return jax.shard_map(
        body,
        mesh=mesh,
        in_specs=(P(("groups", "rows"), None),) * 2 + (P(),) * 15,
        out_specs=P(("groups", "rows"), None, None),
        check_vma=False,
    )
```

```python
import functools

import jax
import jax.numpy as jnp
from jax import lax
from jax.experimental import pallas as pl
from jax.experimental.pallas import tpu as pltpu
from jax.sharding import PartitionSpec as P

GW = 192
BF16 = jnp.bfloat16
F32 = jnp.float32

PIECES = 2
PJ_SIB, PJ_THREE, CO_SIB, CO_ONE, CO_TWO, S_REA, S_IN1, S_MER, S_FAR = range(9)
PJ_ONE = 9
PJ_TWO = PJ_ONE + PIECES
KINDS = PJ_TWO + PIECES
STRIP = 64


def dot(a, b):
    return jnp.dot(a, b, preferred_element_type=F32)


def put(slab, row, even, odd):
    width, chans = even.shape
    at = lax.broadcasted_iota(jnp.int32, even.shape, 0)
    before = jnp.where(at == 0, 0.0, pltpu.roll(odd, 1, 0)).astype(BF16)
    after = jnp.where(at == width - 1, 0.0, pltpu.roll(even, width - 1, 0)).astype(BF16)
    even, odd = even.astype(BF16), odd.astype(BF16)
    for group, value in enumerate((before - odd, even + odd, even - after, odd - even)):
        slab[row, :, group * chans : (group + 1) * chans] = value


def prepare(weight):
    depth = weight.shape[2]

    def strip(step, carry):
        rows = pl.ds(pl.multiple_of(step * STRIP, STRIP), STRIP)
        for k in range(3):
            outer = 0.5 * (weight[0, k, rows, :].astype(F32) + weight[2, k, rows, :].astype(F32))
            inner = 0.5 * weight[1, k, rows, :].astype(F32)
            weight[1, k, rows, :] = (outer + inner).astype(BF16)
            weight[3, k, rows, :] = (outer - inner).astype(BF16)
        return carry

    lax.fori_loop(0, depth // STRIP, strip, 0)


def kernel(
    count,
    tap_h,
    coarse_h,
    proj_h,
    proj_bh,
    lift_h,
    lift_bh,
    merge_h,
    out_h,
    out_bh,
    fi_h,
    fi_bh,
    fo_h,
    fo_bh,
    si_h,
    si_bh,
    so_h,
    so_bh,
    result,
    tap,
    coarse,
    proj_w,
    proj_b,
    lift_w,
    lift_b,
    merge_w,
    out_w,
    out_b,
    fi_w,
    fi_b,
    fo_w,
    fo_b,
    si_w,
    si_b,
    so_w,
    so_b,
    pj,
    wid,
    rea,
    rea_raw,
    carried,
    in1,
    mer,
    mer_raw,
    in2,
    local_sem,
    send_sem,
    recv_sem,
):
    width = tap.shape[0]
    feat = proj_w.shape[1]
    chans = out_w.shape[1]
    me = lax.axis_index("rows")
    side = lax.rem(me, 2)
    step = 2 * side - 1
    sibling = me - step

    def inside(device):
        return jnp.logical_and(device >= 0, device < count)

    valid = (True, inside(me + step), inside(me + 2 * step), inside(me + 3 * step))
    back_two = inside(me - 2 * step)

    started = []

    def fetch(src, dst):
        copy = pltpu.make_async_copy(src, dst, local_sem.at[len(started)])
        started.append(copy)
        copy.start()
        return [copy]

    def fetch_conv(src, dst):
        copies = []
        for k in range(3):
            copies += fetch(src.at[side * k + (1 - side) * (2 - k)], dst.at[pl.ds(0, 3), k])
        return copies

    def done(copies):
        for copy in copies:
            copy.wait()

    tap_in = fetch(tap_h, tap) + fetch(proj_h, proj_w) + fetch(proj_bh, proj_b)
    coarse_in = fetch(coarse_h, coarse.at[0])
    lift_in = fetch(lift_bh, lift_b)
    half = 2 * feat
    for m in range(2):
        where = pl.multiple_of((side * m + (1 - side) * (1 - m)) * half, half)
        lift_in += fetch(lift_h.at[:, pl.ds(where, half)], lift_w.at[:, pl.ds(m * half, half)])

    partners = (
        (me + step, valid[1]),
        (me + 2 * step, valid[2]),
        (me - 2 * step, back_two),
        (me + 3 * step, valid[3]),
    )
    barrier = pltpu.get_barrier_semaphore()
    expected = jnp.int32(1)
    pl.semaphore_signal(
        barrier, inc=1, device_id={"rows": sibling}, device_id_type=pl.DeviceIdType.MESH
    )
    for device, there in partners:

        @pl.when(there)
        def _():
            pl.semaphore_signal(
                barrier, inc=1, device_id={"rows": device}, device_id_type=pl.DeviceIdType.MESH
            )

        expected = expected + there.astype(jnp.int32)

    def remote(src, dst, kind, device):
        return pltpu.make_async_remote_copy(
            src_ref=src,
            dst_ref=dst,
            send_sem=send_sem.at[kind],
            recv_sem=recv_sem.at[kind],
            device_id={"rows": device},
            device_id_type=pl.DeviceIdType.MESH,
        )

    sent = []

    def send(src, dst, kind, device, there=None):
        sent.append((remote(src, dst, kind, device), there))
        if there is None:
            sent[-1][0].start()
        else:
            pl.when(there)(sent[-1][0].start)

    def received(dst, kind, there=None):
        copy = remote(dst, dst, kind, sibling)
        if there is None:
            copy.wait_recv()
        else:
            pl.when(there)(copy.wait_recv)

    done(tap_in)
    merge_in = fetch_conv(merge_h, merge_w)
    out_in = fetch(out_h, out_w) + fetch(out_bh, out_b)
    fi_in = fetch(fi_bh, fi_b) + fetch_conv(fi_h, fi_w)
    fo_in = fetch(fo_bh, fo_b) + fetch_conv(fo_h, fo_w)
    si_in = fetch(si_bh, si_b) + fetch_conv(si_h, si_w)
    so_in = fetch(so_bh, so_b) + fetch_conv(so_h, so_w)
    pj[0] = (dot(tap[...], proj_w[...]) + proj_b[...]).astype(BF16)

    piece = width // PIECES

    def part(slot, k):
        return pj.at[slot, pl.ds(k * piece, piece)]

    pl.semaphore_wait(barrier, expected)
    at_end = jnp.logical_and(back_two, jnp.logical_not(valid[1]))
    for k in range(PIECES):
        send(part(0, k), part(1, k), PJ_ONE + k, me + step, valid[1])
        send(part(0, k), part(2, k), PJ_TWO + k, me - 2 * step, at_end)
    send(pj.at[0], pj.at[4], PJ_SIB, sibling)
    done(coarse_in)
    send(coarse.at[0], coarse.at[3], CO_SIB, sibling)

    def pass_on(k):
        received(part(1, k), PJ_ONE + k, valid[1])
        send(part(1, k), part(2, k), PJ_TWO + k, me + 3 * step, valid[3])

    def lift(token, slab_token, halves):
        for m in halves:
            both = dot(pj[slab_token], lift_w[:, m * half : (m + 1) * half])
            even = both[:, :feat] + lift_b[...]
            odd = both[:, feat:] + lift_b[...]
            if token > 0:
                even = jnp.where(valid[token], even, 0.0)
                odd = jnp.where(valid[token], odd, 0.0)
            put(wid, 2 * token + m + 1, even, odd)

    def conv(slab, weight, low, high, base=1):
        group = slab.shape[2] // 4
        rows = high - low
        products = []
        for place in range(4):
            cells = [
                slab[low + base - 1 + k : high + base - 1 + k, :, place * group : (place + 1) * group]
                .reshape(rows * width, group)
                for k in range(3)
            ]
            taps = weight[place].reshape(3 * group, chans)
            products.append(dot(jnp.concatenate(cells, axis=1), taps))
        first, total, last, spread = products
        even = (total + spread) + first
        odd = (total - spread) - last
        return even.reshape(rows, width, chans), odd.reshape(rows, width, chans)

    def keep(row, value):
        return value if row < 2 else jnp.where(valid[row // 2], value, 0.0)

    def merge_rows(low, high):
        even, odd = conv(wid, merge_w, low, high)
        for row in range(low, high):
            e, o = keep(row, even[row - low]), keep(row, odd[row - low])
            if row < 4:
                rea_raw[row, :, :chans] = e.astype(BF16)
                rea_raw[row, :, chans:] = o.astype(BF16)
            put(rea, row + 1, jnp.maximum(e, 0.0), jnp.maximum(o, 0.0))

    def inner_rows(src, weight, bias, dst, low, high, base=1):
        even, odd = conv(src, weight, low, high, base)
        for row in range(low, high):
            e = jnp.maximum(even[row - low] + bias[...], 0.0)
            o = jnp.maximum(odd[row - low] + bias[...], 0.0)
            put(dst, row + 1, keep(row, e), keep(row, o))

    def merged_rows(low, high):
        even, odd = conv(in1, fo_w, low, high)
        for row in range(low, high):
            outer = []
            for parity, value in enumerate((even, odd)):
                lanes = slice(parity * chans, (parity + 1) * chans)
                whole = (
                    value[row - low]
                    + fo_b[...]
                    + rea_raw[row, :, lanes].astype(F32)
                    + carried[row, :, lanes]
                )
                whole = keep(row, whole)
                if row < 2:
                    mer_raw[row, :, lanes] = whole.astype(BF16)
                outer.append(jnp.maximum(whole, 0.0))
            put(mer, row + 2, *outer)

    def carry(row, near, far):
        band = 0.75 * coarse[near].astype(F32) + 0.25 * coarse[far].astype(F32)
        at = lax.broadcasted_iota(jnp.int32, band.shape, 0)
        before = jnp.where(at == 0, band, pltpu.roll(band, 1, 0))
        after = jnp.where(at == width - 1, band, pltpu.roll(band, width - 1, 0))
        for parity, other in enumerate((before, after)):
            spread = (0.75 * band + 0.25 * other).astype(BF16)
            carried[row, :, parity * chans : (parity + 1) * chans] = (
                dot(spread, out_w[...]) + out_b[...]
            )

    done(lift_in)
    lift(0, 0, (0, 1))
    send(pj.at[0], pj.at[3], PJ_THREE, me + 3 * step, valid[3])
    send(coarse.at[0], coarse.at[1], CO_ONE, me + step, valid[1])
    send(coarse.at[0], coarse.at[2], CO_TWO, me - 2 * step, at_end)
    done(merge_in)
    prepare(merge_w)
    received(pj.at[4], PJ_SIB)
    lift(-1, 4, (1,))
    merge_rows(0, 1)
    send(rea.at[1], rea.at[0], S_REA, sibling)

    done(out_in)
    received(coarse.at[3], CO_SIB)
    carry(0, 0, 3)
    done(fi_in)
    prepare(fi_w)
    done(fo_in)
    prepare(fo_w)
    pass_on(0)
    done(si_in)
    prepare(si_w)
    done(so_in)
    prepare(so_w)
    for k in range(1, PIECES):
        pass_on(k)

    @pl.when(jnp.logical_not(valid[1]))
    def _():
        coarse[1] = coarse[0]
        pj[1] = jnp.zeros_like(pj[1])

    lift(1, 1, (0, 1))
    merge_rows(1, 3)
    received(rea.at[0], S_REA)
    inner_rows(rea, fi_w, fi_b, in1, 0, 1)
    send(in1.at[1], in1.at[0], S_IN1, sibling)
    received(coarse.at[1], CO_ONE, valid[1])
    send(coarse.at[1], coarse.at[2], CO_TWO, me + 3 * step, valid[3])
    inner_rows(rea, fi_w, fi_b, in1, 1, 2)
    carry(1, 0, 1)
    carry(2, 1, 0)

    @pl.when(jnp.logical_not(valid[2]))
    def _():
        pj[2] = jnp.zeros_like(pj[2])

    @pl.when(jnp.logical_not(valid[3]))
    def _():
        pj[3] = jnp.zeros_like(pj[3])

    received(pj.at[3], PJ_THREE, valid[3])
    lift(3, 3, (0,))
    for k in range(PIECES):
        received(part(2, k), PJ_TWO + k, valid[2])
    lift(2, 2, (0, 1))
    merge_rows(3, 6)
    inner_rows(rea, fi_w, fi_b, in1, 2, 5)
    received(in1.at[0], S_IN1)
    merged_rows(0, 2)
    send(mer.at[2], mer.at[1], S_MER, sibling)
    send(mer.at[3], mer.at[0], S_FAR, sibling)

    @pl.when(jnp.logical_not(valid[2]))
    def _():
        coarse[2] = coarse[1]

    received(coarse.at[2], CO_TWO, valid[2])
    carry(3, 1, 2)
    merged_rows(2, 4)
    inner_rows(mer, si_w, si_b, in2, 1, 3, 2)
    received(mer.at[1], S_MER)
    received(mer.at[0], S_FAR)
    inner_rows(mer, si_w, si_b, in2, -1, 1, 2)

    line = lax.broadcasted_iota(jnp.int32, (2 * width, 2 * width), 0)
    column = lax.broadcasted_iota(jnp.int32, (2 * width, 2 * width), 1)
    weave = (column == line // 2 + width * (line % 2)).astype(F32).astype(BF16)
    for row in (1, 0):
        sides = conv(in2, so_w, row, row + 1)
        united = [
            (sides[parity][0] + so_b[...] + mer_raw[row, :, parity * chans : (parity + 1) * chans].astype(F32)).astype(BF16)
            for parity in range(2)
        ]
        woven = dot(weave, jnp.concatenate(united, axis=0)).astype(BF16)
        target = side * row + (1 - side) * (1 - row)
        result[pl.ds(target, 1)] = woven[None]

    for copy, there in sent:
        if there is None:
            copy.wait_send()
        else:
            pl.when(there)(copy.wait_send)


def body(*args):
    count = lax.axis_size("rows")
    tap_two, coarse_path, proj_weight = args[:3]
    tokens, depth = tap_two.shape
    feat, chans = proj_weight.shape[1], coarse_path.shape[1]
    assert tokens == GW and count % 2 == 0
    convs = (6, 9, 11, 13, 15)
    args = [arg.reshape(1, -1) if arg.ndim == 1 else arg for arg in args]
    args = [
        arg.reshape(3, 3, arg.shape[0] // 9, chans) if place in convs else arg
        for place, arg in enumerate(args)
    ]

    scratch = []
    for place, arg in enumerate(args):
        shape = (4, *arg.shape) if place == 1 else arg.shape
        shape = (4, *shape[1:]) if place in convs else shape
        scratch.append(pltpu.VMEM(shape, arg.dtype))
    scratch += [
        pltpu.VMEM((5, tokens, feat), BF16),
        pltpu.VMEM((8, tokens, 4 * feat), BF16),
        pltpu.VMEM((7, tokens, 4 * chans), BF16),
        pltpu.VMEM((4, tokens, 2 * chans), BF16),
        pltpu.VMEM((4, tokens, 2 * chans), F32),
        pltpu.VMEM((6, tokens, 4 * chans), BF16),
        pltpu.VMEM((6, tokens, 4 * chans), BF16),
        pltpu.VMEM((2, tokens, 2 * chans), BF16),
        pltpu.VMEM((4, tokens, 4 * chans), BF16),
        pltpu.SemaphoreType.DMA((28,)),
        pltpu.SemaphoreType.DMA((KINDS,)),
        pltpu.SemaphoreType.DMA((KINDS,)),
    ]
    mid = pl.pallas_call(
        functools.partial(kernel, count),
        out_shape=pltpu.VMEM((2, 2 * tokens, chans), BF16),
        in_specs=[pl.BlockSpec(memory_space=pl.ANY)] * len(args),
        out_specs=pl.BlockSpec(memory_space=pltpu.VMEM),
        scratch_shapes=scratch,
        compiler_params=pltpu.CompilerParams(
            collective_id=0, has_side_effects=True, vmem_limit_bytes=60 * 2**20
        ),
        name="fused_tap",
    )(*args)

    return mid


def solution(mesh):
    return jax.shard_map(
        body,
        mesh=mesh,
        in_specs=(P(("groups", "rows"), None),) * 2 + (P(),) * 15,
        out_specs=P(("groups", "rows"), None, None),
        check_vma=False,
    )
```

```python
import functools

import jax
import jax.numpy as jnp
from jax import lax
from jax.experimental import pallas as pl
from jax.experimental.pallas import tpu as pltpu
from jax.sharding import PartitionSpec as P

GW = 192
BF16 = jnp.bfloat16
F32 = jnp.float32

PIECES = 2
PJ_SIB, PJ_THREE, CO_SIB, CO_ONE, CO_TWO, S_REA, S_IN1, S_MER, S_FAR = range(9)
PJ_ONE = 9
PJ_TWO = PJ_ONE + PIECES
KINDS = PJ_TWO + PIECES
STRIP = 64
LANES = 128


def dot(a, b):
    return jnp.dot(a, b, preferred_element_type=F32)


def put(slab, row, even, odd):
    width, chans = even.shape
    at = lax.broadcasted_iota(jnp.int32, even.shape, 0)
    before = jnp.where(at == 0, 0.0, pltpu.roll(odd, 1, 0)).astype(BF16)
    after = jnp.where(at == width - 1, 0.0, pltpu.roll(even, width - 1, 0)).astype(BF16)
    even, odd = even.astype(BF16), odd.astype(BF16)
    for group, value in enumerate((before - odd, even + odd, even - after, odd - even)):
        slab[row, :, group * chans : (group + 1) * chans] = value


def prepare(weight):
    depth = weight.shape[2]

    def strip(step, carry):
        rows = pl.ds(pl.multiple_of(step * STRIP, STRIP), STRIP)
        for k in range(3):
            outer = 0.5 * (weight[0, k, rows, :].astype(F32) + weight[2, k, rows, :].astype(F32))
            inner = 0.5 * weight[1, k, rows, :].astype(F32)
            weight[1, k, rows, :] = (outer + inner).astype(BF16)
            weight[3, k, rows, :] = (outer - inner).astype(BF16)
        return carry

    lax.fori_loop(0, depth // STRIP, strip, 0)


def kernel(
    count,
    tap_h,
    coarse_h,
    proj_h,
    proj_bh,
    lift_h,
    lift_bh,
    merge_h,
    out_h,
    out_bh,
    fi_h,
    fi_bh,
    fo_h,
    fo_bh,
    si_h,
    si_bh,
    so_h,
    so_bh,
    result,
    tap,
    coarse,
    proj_w,
    proj_b,
    lift_w,
    lift_b,
    merge_w,
    out_w,
    out_b,
    fi_w,
    fi_b,
    fo_w,
    fo_b,
    si_w,
    si_b,
    so_w,
    so_b,
    pj,
    wid,
    rea,
    rea_raw,
    carried,
    in1,
    mer,
    mer_raw,
    in2,
    woven,
    local_sem,
    send_sem,
    recv_sem,
):
    width = tap.shape[0]
    feat = proj_w.shape[1]
    chans = out_w.shape[1]
    me = lax.axis_index("rows")
    side = lax.rem(me, 2)
    step = 2 * side - 1
    sibling = me - step

    def inside(device):
        return jnp.logical_and(device >= 0, device < count)

    valid = (True, inside(me + step), inside(me + 2 * step), inside(me + 3 * step))
    back_two = inside(me - 2 * step)

    started = []

    def fetch(src, dst):
        copy = pltpu.make_async_copy(src, dst, local_sem.at[len(started)])
        started.append(copy)
        copy.start()
        return [copy]

    def fetch_conv(src, dst):
        sem = local_sem.at[len(started)]
        for k in range(3):
            pltpu.make_async_copy(
                src.at[side * k + (1 - side) * (2 - k)], dst.at[pl.ds(0, 3), k], sem
            ).start()
        landed = dst.at[pl.ds(0, 3)]
        started.append(pltpu.make_async_copy(landed, landed, sem))
        return [started[-1]]

    def done(copies):
        for copy in copies:
            copy.wait()

    tap_in = fetch(tap_h, tap) + fetch(proj_h, proj_w) + fetch(proj_bh, proj_b)
    coarse_in = fetch(coarse_h, coarse.at[0])
    lift_in = fetch(lift_bh, lift_b)
    half = 2 * feat
    lift_sem = local_sem.at[len(started)]
    for m in range(2):
        where = pl.multiple_of((side * m + (1 - side) * (1 - m)) * half, half)
        pltpu.make_async_copy(
            lift_h.at[:, pl.ds(where, half)], lift_w.at[:, pl.ds(m * half, half)], lift_sem
        ).start()
    started.append(pltpu.make_async_copy(lift_w, lift_w, lift_sem))
    lift_in.append(started[-1])

    partners = (
        (me + step, valid[1]),
        (me + 2 * step, valid[2]),
        (me - 2 * step, back_two),
        (me + 3 * step, valid[3]),
    )
    barrier = pltpu.get_barrier_semaphore()
    expected = jnp.int32(1)
    pl.semaphore_signal(
        barrier, inc=1, device_id={"rows": sibling}, device_id_type=pl.DeviceIdType.MESH
    )
    for device, there in partners:

        @pl.when(there)
        def _():
            pl.semaphore_signal(
                barrier, inc=1, device_id={"rows": device}, device_id_type=pl.DeviceIdType.MESH
            )

        expected = expected + there.astype(jnp.int32)

    def remote(src, dst, kind, device):
        return pltpu.make_async_remote_copy(
            src_ref=src,
            dst_ref=dst,
            send_sem=send_sem.at[kind],
            recv_sem=recv_sem.at[kind],
            device_id={"rows": device},
            device_id_type=pl.DeviceIdType.MESH,
        )

    sent = []

    def send(src, dst, kind, device, there=None):
        sent.append((remote(src, dst, kind, device), there))
        if there is None:
            sent[-1][0].start()
        else:
            pl.when(there)(sent[-1][0].start)

    def received(dst, kind, there=None):
        copy = remote(dst, dst, kind, sibling)
        if there is None:
            copy.wait_recv()
        else:
            pl.when(there)(copy.wait_recv)

    done(tap_in)
    merge_in = fetch_conv(merge_h, merge_w)
    out_in = fetch(out_h, out_w) + fetch(out_bh, out_b)
    fi_in = fetch(fi_bh, fi_b) + fetch_conv(fi_h, fi_w)
    fo_in = fetch(fo_bh, fo_b) + fetch_conv(fo_h, fo_w)
    si_in = fetch(si_bh, si_b) + fetch_conv(si_h, si_w)
    so_in = fetch(so_bh, so_b) + fetch_conv(so_h, so_w)
    pj[0] = (dot(tap[...], proj_w[...]) + proj_b[...]).astype(BF16)

    piece = width // PIECES

    def part(slot, k):
        return pj.at[slot, pl.ds(k * piece, piece)]

    pl.semaphore_wait(barrier, expected)
    at_end = jnp.logical_and(back_two, jnp.logical_not(valid[1]))
    to_end = jnp.logical_and(
        jnp.logical_and(back_two, valid[1]), jnp.logical_not(inside(me - 4 * step))
    )
    relays = jnp.logical_and(valid[3], inside(me + 5 * step))
    for k in range(PIECES):
        send(part(0, k), part(1, k), PJ_ONE + k, me + step, valid[1])
    for k in range(PIECES):
        send(part(0, k), part(2, k), PJ_TWO + k, me - 2 * step, to_end)
    send(pj.at[0], pj.at[4], PJ_SIB, sibling)
    done(coarse_in)
    send(coarse.at[0], coarse.at[3], CO_SIB, sibling)

    def pass_on(k):
        received(part(1, k), PJ_ONE + k, valid[1])
        send(part(1, k), part(2, k), PJ_TWO + k, me + 3 * step, relays)

    def lift(token, slab_token, halves):
        for m in halves:
            both = dot(pj[slab_token], lift_w[:, m * half : (m + 1) * half])
            even = both[:, :feat] + lift_b[...]
            odd = both[:, feat:] + lift_b[...]
            if token > 0:
                even = jnp.where(valid[token], even, 0.0)
                odd = jnp.where(valid[token], odd, 0.0)
            put(wid, 2 * token + m + 1, even, odd)

    def conv(slab, weight, low, high, base=1):
        group = slab.shape[2] // 4
        rows = high - low
        products = []
        for place in range(4):
            cells = [
                slab[low + base - 1 + k : high + base - 1 + k, :, place * group : (place + 1) * group]
                .reshape(rows * width, group)
                for k in range(3)
            ]
            taps = weight[place].reshape(3 * group, chans)
            products.append(dot(jnp.concatenate(cells, axis=1), taps))
        first, total, last, spread = products
        even = (total + spread) + first
        odd = (total - spread) - last
        return even.reshape(rows, width, chans), odd.reshape(rows, width, chans)

    def keep(row, value):
        return value if row < 2 else jnp.where(valid[row // 2], value, 0.0)

    def merge_rows(low, high):
        even, odd = conv(wid, merge_w, low, high)
        for row in range(low, high):
            e, o = keep(row, even[row - low]), keep(row, odd[row - low])
            if row < 4:
                rea_raw[row, :, :chans] = e.astype(BF16)
                rea_raw[row, :, chans:] = o.astype(BF16)
            put(rea, row + 1, jnp.maximum(e, 0.0), jnp.maximum(o, 0.0))

    def inner_rows(src, weight, bias, dst, low, high, base=1):
        even, odd = conv(src, weight, low, high, base)
        for row in range(low, high):
            e = jnp.maximum(even[row - low] + bias[...], 0.0)
            o = jnp.maximum(odd[row - low] + bias[...], 0.0)
            put(dst, row + 1, keep(row, e), keep(row, o))

    def merged_rows(low, high):
        even, odd = conv(in1, fo_w, low, high)
        for row in range(low, high):
            outer = []
            for parity, value in enumerate((even, odd)):
                lanes = slice(parity * chans, (parity + 1) * chans)
                whole = (
                    value[row - low]
                    + fo_b[...]
                    + rea_raw[row, :, lanes].astype(F32)
                    + carried[row, :, lanes]
                )
                whole = keep(row, whole)
                if row < 2:
                    mer_raw[row, :, lanes] = whole.astype(BF16)
                outer.append(jnp.maximum(whole, 0.0))
            put(mer, row + 2, *outer)

    def carry(row, near, far):
        other = coarse[far].astype(F32)
        if row == 1:
            other = jnp.where(valid[1], other, coarse[near].astype(F32))
        band = 0.75 * coarse[near].astype(F32) + 0.25 * other
        at = lax.broadcasted_iota(jnp.int32, band.shape, 0)
        before = jnp.where(at == 0, band, pltpu.roll(band, 1, 0))
        after = jnp.where(at == width - 1, band, pltpu.roll(band, width - 1, 0))
        for parity, other in enumerate((before, after)):
            spread = (0.75 * band + 0.25 * other).astype(BF16)
            carried[row, :, parity * chans : (parity + 1) * chans] = (
                dot(spread, out_w[...]) + out_b[...]
            )

    def merge_row(row):
        merge_rows(row, row + 1)

    def first_row(row):
        inner_rows(rea, fi_w, fi_b, in1, row, row + 1)

    def merged_row(row):
        merged_rows(row, row + 1)

    def second_row(row):
        inner_rows(mer, si_w, si_b, in2, row, row + 1, 2)

    def final_row(row):
        even, odd = conv(in2, so_w, row, row + 1)
        for parity, value in enumerate((even[0], odd[0])):
            lanes = slice(parity * chans, (parity + 1) * chans)
            united = value + so_b[...] + mer_raw[row, :, lanes].astype(F32)
            for block in range(chans // LANES):
                cells = united[:, block * LANES : (block + 1) * LANES]
                woven[row, block, pl.ds(parity, width, stride=2), :] = cells
        target = side * row + (1 - side) * (1 - row)
        for block in range(chans // LANES):
            lanes = slice(block * LANES, (block + 1) * LANES)
            result[pl.ds(target, 1), :, lanes] = woven[row, block].astype(BF16)[None]

    done(lift_in)
    lift(0, 0, (0, 1))
    send(pj.at[0], pj.at[3], PJ_THREE, me + 3 * step, valid[3])
    done(merge_in)
    prepare(merge_w)
    received(pj.at[4], PJ_SIB)
    lift(-1, 4, (1,))
    merge_row(0)
    send(rea.at[1], rea.at[0], S_REA, sibling)
    done(out_in)
    received(coarse.at[3], CO_SIB)
    carry(0, 0, 3)
    done(fi_in)
    prepare(fi_w)
    for k in range(PIECES):
        send(part(0, k), part(2, k), PJ_TWO + k, me - 2 * step, at_end)
    pass_on(0)
    done(fo_in)
    prepare(fo_w)
    done(si_in)
    prepare(si_w)
    done(so_in)
    prepare(so_w)
    received(rea.at[0], S_REA)
    pass_on(1)

    lift(1, 1, (0, 1))
    merge_row(1)
    merge_row(2)
    first_row(0)
    first_row(1)
    send(in1.at[1], in1.at[0], S_IN1, sibling)
    send(coarse.at[0], coarse.at[1], CO_ONE, me + step, valid[1])
    send(coarse.at[0], coarse.at[2], CO_TWO, me - 2 * step, back_two)
    received(pj.at[3], PJ_THREE, valid[3])
    lift(3, 3, (0,))

    for k in range(PIECES):
        received(part(2, k), PJ_TWO + k, valid[2])
    lift(2, 2, (0, 1))
    merge_row(3)
    merge_row(4)
    first_row(2)
    received(in1.at[0], S_IN1)
    merged_row(0)
    merge_row(5)
    first_row(3)
    send(mer.at[2], mer.at[1], S_MER, sibling)
    first_row(4)
    received(coarse.at[1], CO_ONE, valid[1])
    received(coarse.at[2], CO_TWO, valid[2])
    carry(1, 0, 1)
    merged_row(1)
    carry(2, 1, 0)
    send(mer.at[3], mer.at[0], S_FAR, sibling)
    merged_row(2)
    carry(3, 1, 2)
    second_row(1)
    merged_row(3)
    second_row(2)
    received(mer.at[1], S_MER)
    received(mer.at[0], S_FAR)
    second_row(0)
    second_row(-1)
    final_row(1)
    final_row(0)

    for copy, there in sent:
        if there is None:
            copy.wait_send()
        else:
            pl.when(there)(copy.wait_send)


def body(*args):
    count = lax.axis_size("rows")
    tap_two, coarse_path, proj_weight = args[:3]
    tokens, depth = tap_two.shape
    feat, chans = proj_weight.shape[1], coarse_path.shape[1]
    assert tokens == GW and count % 2 == 0
    convs = (6, 9, 11, 13, 15)
    args = [arg.reshape(1, -1) if arg.ndim == 1 else arg for arg in args]
    args = [
        arg.reshape(3, 3, arg.shape[0] // 9, chans) if place in convs else arg
        for place, arg in enumerate(args)
    ]

    scratch = []
    for place, arg in enumerate(args):
        shape = (4, *arg.shape) if place == 1 else arg.shape
        shape = (4, *shape[1:]) if place in convs else shape
        scratch.append(pltpu.VMEM(shape, arg.dtype))
    scratch += [
        pltpu.VMEM((5, tokens, feat), BF16),
        pltpu.VMEM((8, tokens, 4 * feat), BF16),
        pltpu.VMEM((7, tokens, 4 * chans), BF16),
        pltpu.VMEM((4, tokens, 2 * chans), BF16),
        pltpu.VMEM((4, tokens, 2 * chans), F32),
        pltpu.VMEM((6, tokens, 4 * chans), BF16),
        pltpu.VMEM((6, tokens, 4 * chans), BF16),
        pltpu.VMEM((2, tokens, 2 * chans), BF16),
        pltpu.VMEM((4, tokens, 4 * chans), BF16),
        pltpu.VMEM((2, chans // LANES, 2 * tokens, LANES), F32),
        pltpu.SemaphoreType.DMA((17,)),
        pltpu.SemaphoreType.DMA((KINDS,)),
        pltpu.SemaphoreType.DMA((KINDS,)),
    ]
    mid = pl.pallas_call(
        functools.partial(kernel, count),
        out_shape=pltpu.VMEM((2, 2 * tokens, chans), BF16),
        in_specs=[pl.BlockSpec(memory_space=pl.ANY)] * len(args),
        out_specs=pl.BlockSpec(memory_space=pltpu.VMEM),
        scratch_shapes=scratch,
        compiler_params=pltpu.CompilerParams(
            collective_id=0, has_side_effects=True, vmem_limit_bytes=60 * 2**20
        ),
        name="fused_tap",
    )(*args)

    return mid


def solution(mesh):
    return jax.shard_map(
        body,
        mesh=mesh,
        in_specs=(P(("groups", "rows"), None),) * 2 + (P(),) * 15,
        out_specs=P(("groups", "rows"), None, None),
        check_vma=False,
    )
```

```python
import functools

import jax
import jax.numpy as jnp
from jax import lax
from jax.experimental import pallas as pl
from jax.experimental.pallas import tpu as pltpu
from jax.sharding import PartitionSpec as P

GW = 192
BF16 = jnp.bfloat16
F32 = jnp.float32

PIECES = 2
PJ_SIB, PJ_THREE, CO_SIB, CO_ONE, CO_TWO, S_REA, S_IN1, S_MER, S_FAR = range(9)
PJ_ONE = 9
PJ_TWO = PJ_ONE + PIECES
KINDS = PJ_TWO + PIECES
STRIP = 64
LANES = 128


def dot(a, b):
    return jnp.dot(a, b, preferred_element_type=F32)


def put(slab, row, even, odd):
    width, chans = even.shape
    at = lax.broadcasted_iota(jnp.int32, even.shape, 0)
    before = jnp.where(at == 0, 0.0, pltpu.roll(odd, 1, 0)).astype(BF16)
    after = jnp.where(at == width - 1, 0.0, pltpu.roll(even, width - 1, 0)).astype(BF16)
    even, odd = even.astype(BF16), odd.astype(BF16)
    for group, value in enumerate((before - odd, even + odd, even - after, odd - even)):
        slab[row, :, group * chans : (group + 1) * chans] = value


def prepare(weight):
    depth = weight.shape[2]

    def strip(step, carry):
        rows = pl.ds(pl.multiple_of(step * STRIP, STRIP), STRIP)
        for k in range(3):
            outer = 0.5 * (weight[0, k, rows, :].astype(F32) + weight[2, k, rows, :].astype(F32))
            inner = 0.5 * weight[1, k, rows, :].astype(F32)
            weight[1, k, rows, :] = (outer + inner).astype(BF16)
            weight[3, k, rows, :] = (outer - inner).astype(BF16)
        return carry

    lax.fori_loop(0, depth // STRIP, strip, 0)


def kernel(
    count,
    tap_h,
    coarse_h,
    proj_h,
    proj_bh,
    lift_h,
    lift_bh,
    merge_h,
    out_h,
    out_bh,
    fi_h,
    fi_bh,
    fo_h,
    fo_bh,
    si_h,
    si_bh,
    so_h,
    so_bh,
    result,
    tap,
    coarse,
    proj_w,
    proj_b,
    lift_w,
    lift_b,
    merge_w,
    out_w,
    out_b,
    fi_w,
    fi_b,
    fo_w,
    fo_b,
    si_w,
    si_b,
    so_w,
    so_b,
    pj,
    wid,
    rea,
    rea_raw,
    carried,
    in1,
    mer,
    mer_raw,
    in2,
    woven,
    early,
    local_sem,
    send_sem,
    recv_sem,
):
    width = tap.shape[0]
    feat = proj_w.shape[1]
    chans = out_w.shape[1]
    me = lax.axis_index("rows")
    side = lax.rem(me, 2)
    step = 2 * side - 1
    sibling = me - step

    def inside(device):
        return jnp.logical_and(device >= 0, device < count)

    valid = (True, inside(me + step), inside(me + 2 * step), inside(me + 3 * step))
    back_two = inside(me - 2 * step)

    started = []

    def fetch(src, dst):
        copy = pltpu.make_async_copy(src, dst, local_sem.at[len(started)])
        started.append(copy)
        copy.start()
        return [copy]

    def fetch_conv(src, dst):
        sem = local_sem.at[len(started)]
        for k in range(3):
            pltpu.make_async_copy(
                src.at[side * k + (1 - side) * (2 - k)], dst.at[pl.ds(0, 3), k], sem
            ).start()
        landed = dst.at[pl.ds(0, 3)]
        started.append(pltpu.make_async_copy(landed, landed, sem))
        return [started[-1]]

    def done(copies):
        for copy in copies:
            copy.wait()

    tap_in = fetch(tap_h, tap) + fetch(proj_h, proj_w) + fetch(proj_bh, proj_b)
    coarse_in = fetch(coarse_h, coarse.at[0])
    lift_in = fetch(lift_bh, lift_b)
    half = 2 * feat
    lift_sem = local_sem.at[len(started)]
    for m in range(2):
        where = pl.multiple_of((side * m + (1 - side) * (1 - m)) * half, half)
        pltpu.make_async_copy(
            lift_h.at[:, pl.ds(where, half)], lift_w.at[:, pl.ds(m * half, half)], lift_sem
        ).start()
    started.append(pltpu.make_async_copy(lift_w, lift_w, lift_sem))
    lift_in.append(started[-1])

    partners = (
        (me + step, valid[1]),
        (me + 2 * step, valid[2]),
        (me - 2 * step, back_two),
        (me + 3 * step, valid[3]),
    )
    barrier = pltpu.get_barrier_semaphore()
    expected = jnp.int32(1)
    pl.semaphore_signal(
        barrier, inc=1, device_id={"rows": sibling}, device_id_type=pl.DeviceIdType.MESH
    )
    for device, there in partners:

        @pl.when(there)
        def _():
            pl.semaphore_signal(
                barrier, inc=1, device_id={"rows": device}, device_id_type=pl.DeviceIdType.MESH
            )

        expected = expected + there.astype(jnp.int32)

    def remote(src, dst, kind, device):
        return pltpu.make_async_remote_copy(
            src_ref=src,
            dst_ref=dst,
            send_sem=send_sem.at[kind],
            recv_sem=recv_sem.at[kind],
            device_id={"rows": device},
            device_id_type=pl.DeviceIdType.MESH,
        )

    sent = []

    def send(src, dst, kind, device, there=None):
        sent.append((remote(src, dst, kind, device), there))
        if there is None:
            sent[-1][0].start()
        else:
            pl.when(there)(sent[-1][0].start)

    def received(dst, kind, there=None):
        copy = remote(dst, dst, kind, sibling)
        if there is None:
            copy.wait_recv()
        else:
            pl.when(there)(copy.wait_recv)

    done(tap_in)
    merge_in = fetch_conv(merge_h, merge_w)
    out_in = fetch(out_h, out_w) + fetch(out_bh, out_b)
    fi_in = fetch(fi_bh, fi_b) + fetch_conv(fi_h, fi_w)
    fo_in = fetch(fo_bh, fo_b) + fetch_conv(fo_h, fo_w)
    si_in = fetch(si_bh, si_b) + fetch_conv(si_h, si_w)
    so_in = fetch(so_bh, so_b) + fetch_conv(so_h, so_w)
    pj[0] = (dot(tap[...], proj_w[...]) + proj_b[...]).astype(BF16)

    piece = width // PIECES

    def part(slot, k):
        return pj.at[slot, pl.ds(k * piece, piece)]

    pl.semaphore_wait(barrier, expected)
    at_end = jnp.logical_and(back_two, jnp.logical_not(valid[1]))
    to_end = jnp.logical_and(
        jnp.logical_and(back_two, valid[1]), jnp.logical_not(inside(me - 4 * step))
    )
    relays = jnp.logical_and(valid[3], inside(me + 5 * step))
    for k in range(PIECES):
        send(part(0, k), part(1, k), PJ_ONE + k, me + step, valid[1])
    send(pj.at[0], pj.at[4], PJ_SIB, sibling)
    done(coarse_in)
    send(coarse.at[0], coarse.at[3], CO_SIB, sibling)

    def pass_on(k):
        received(part(1, k), PJ_ONE + k, valid[1])
        send(part(1, k), part(2, k), PJ_TWO + k, me + 3 * step, relays)

    def lift(token, slab_token, halves):
        for m in halves:
            both = dot(pj[slab_token], lift_w[:, m * half : (m + 1) * half])
            even = both[:, :feat] + lift_b[...]
            odd = both[:, feat:] + lift_b[...]
            if token > 0:
                even = jnp.where(valid[token], even, 0.0)
                odd = jnp.where(valid[token], odd, 0.0)
            put(wid, 2 * token + m + 1, even, odd)

    def product(slab, weight, row, place, low, high):
        group = slab.shape[2] // 4
        lanes = slice(place * group, (place + 1) * group)
        cells = [slab[row + k, :, lanes] for k in range(low, high)]
        taps = weight[place, low:high].reshape((high - low) * group, chans)
        return dot(jnp.concatenate(cells, axis=1), taps)

    early_taps = {1: 2, 2: 1, 3: 2}

    def ahead(row):
        for place in range(4):
            early[(row - 1) % 2, place] = product(wid, merge_w, row, place, 0, early_taps[row])

    def conv(slab, weight, low, high, base=1):
        rows = high - low
        known = early_taps.get(low, 0) if slab is wid else 0
        products = []
        for place in range(4):
            if known:
                late = product(slab, weight, low, place, known, 3)
                products.append(late + early[(low - 1) % 2, place])
            else:
                products.append(product(slab, weight, low + base - 1, place, 0, 3))
        first, total, last, spread = products
        even = (total + spread) + first
        odd = (total - spread) - last
        return even.reshape(rows, width, chans), odd.reshape(rows, width, chans)

    def keep(row, value):
        return value if row < 2 else jnp.where(valid[row // 2], value, 0.0)

    def merge_rows(low, high):
        even, odd = conv(wid, merge_w, low, high)
        for row in range(low, high):
            e, o = keep(row, even[row - low]), keep(row, odd[row - low])
            if row < 4:
                rea_raw[row, :, :chans] = e.astype(BF16)
                rea_raw[row, :, chans:] = o.astype(BF16)
            put(rea, row + 1, jnp.maximum(e, 0.0), jnp.maximum(o, 0.0))

    def inner_rows(src, weight, bias, dst, low, high, base=1):
        even, odd = conv(src, weight, low, high, base)
        for row in range(low, high):
            e = jnp.maximum(even[row - low] + bias[...], 0.0)
            o = jnp.maximum(odd[row - low] + bias[...], 0.0)
            put(dst, row + 1, keep(row, e), keep(row, o))

    def merged_rows(low, high):
        even, odd = conv(in1, fo_w, low, high)
        for row in range(low, high):
            outer = []
            for parity, value in enumerate((even, odd)):
                lanes = slice(parity * chans, (parity + 1) * chans)
                whole = (
                    value[row - low]
                    + fo_b[...]
                    + rea_raw[row, :, lanes].astype(F32)
                    + carried[row, :, lanes]
                )
                whole = keep(row, whole)
                if row < 2:
                    mer_raw[row, :, lanes] = whole.astype(BF16)
                outer.append(jnp.maximum(whole, 0.0))
            put(mer, row + 2, *outer)

    def carry(row, near, far):
        other = coarse[far].astype(F32)
        if row == 1:
            other = jnp.where(valid[1], other, coarse[near].astype(F32))
        band = 0.75 * coarse[near].astype(F32) + 0.25 * other
        at = lax.broadcasted_iota(jnp.int32, band.shape, 0)
        before = jnp.where(at == 0, band, pltpu.roll(band, 1, 0))
        after = jnp.where(at == width - 1, band, pltpu.roll(band, width - 1, 0))
        for parity, other in enumerate((before, after)):
            spread = (0.75 * band + 0.25 * other).astype(BF16)
            carried[row, :, parity * chans : (parity + 1) * chans] = (
                dot(spread, out_w[...]) + out_b[...]
            )

    def merge_row(row):
        merge_rows(row, row + 1)

    def first_row(row):
        inner_rows(rea, fi_w, fi_b, in1, row, row + 1)

    def merged_row(row):
        merged_rows(row, row + 1)

    def second_row(row):
        inner_rows(mer, si_w, si_b, in2, row, row + 1, 2)

    def final_row(row):
        even, odd = conv(in2, so_w, row, row + 1)
        for parity, value in enumerate((even[0], odd[0])):
            lanes = slice(parity * chans, (parity + 1) * chans)
            united = value + so_b[...] + mer_raw[row, :, lanes].astype(F32)
            for block in range(chans // LANES):
                cells = united[:, block * LANES : (block + 1) * LANES]
                woven[row, block, pl.ds(parity, width, stride=2), :] = cells
        target = side * row + (1 - side) * (1 - row)
        for block in range(chans // LANES):
            lanes = slice(block * LANES, (block + 1) * LANES)
            result[pl.ds(target, 1), :, lanes] = woven[row, block].astype(BF16)[None]

    done(lift_in)
    lift(0, 0, (0, 1))
    send(pj.at[0], pj.at[3], PJ_THREE, me + 3 * step, valid[3])
    done(merge_in)
    prepare(merge_w)
    received(pj.at[4], PJ_SIB)
    lift(-1, 4, (1,))
    for k in range(PIECES):
        send(part(0, k), part(2, k), PJ_TWO + k, me - 2 * step, to_end)
    merge_row(0)
    send(rea.at[1], rea.at[0], S_REA, sibling)
    done(out_in)
    received(coarse.at[3], CO_SIB)
    carry(0, 0, 3)
    done(fi_in)
    prepare(fi_w)
    ahead(1)
    ahead(2)
    pass_on(0)
    done(fo_in)
    prepare(fo_w)
    done(si_in)
    prepare(si_w)
    done(so_in)
    prepare(so_w)
    received(rea.at[0], S_REA)
    pass_on(1)
    for k in range(PIECES):
        send(part(0, k), part(2, k), PJ_TWO + k, me - 2 * step, at_end)
    lift(1, 1, (0, 1))
    merge_row(1)
    merge_row(2)
    first_row(0)
    first_row(1)
    send(in1.at[1], in1.at[0], S_IN1, sibling)
    send(coarse.at[0], coarse.at[1], CO_ONE, me + step, valid[1])
    send(coarse.at[0], coarse.at[2], CO_TWO, me - 2 * step, back_two)
    received(pj.at[3], PJ_THREE, valid[3])
    lift(3, 3, (0,))
    ahead(3)

    for k in range(PIECES):
        received(part(2, k), PJ_TWO + k, valid[2])
    lift(2, 2, (0, 1))
    merge_row(3)
    merge_row(4)
    first_row(2)
    received(in1.at[0], S_IN1)
    merged_row(0)
    merge_row(5)
    first_row(3)
    send(mer.at[2], mer.at[1], S_MER, sibling)
    first_row(4)
    received(coarse.at[1], CO_ONE, valid[1])
    received(coarse.at[2], CO_TWO, valid[2])
    carry(1, 0, 1)
    merged_row(1)
    carry(2, 1, 0)
    send(mer.at[3], mer.at[0], S_FAR, sibling)
    merged_row(2)
    carry(3, 1, 2)
    second_row(1)
    merged_row(3)
    second_row(2)
    received(mer.at[1], S_MER)
    received(mer.at[0], S_FAR)
    second_row(0)
    second_row(-1)
    final_row(1)
    final_row(0)

    for copy, there in sent:
        if there is None:
            copy.wait_send()
        else:
            pl.when(there)(copy.wait_send)


def body(*args):
    count = lax.axis_size("rows")
    tap_two, coarse_path, proj_weight = args[:3]
    tokens, depth = tap_two.shape
    feat, chans = proj_weight.shape[1], coarse_path.shape[1]
    assert tokens == GW and count % 2 == 0
    convs = (6, 9, 11, 13, 15)
    args = [arg.reshape(1, -1) if arg.ndim == 1 else arg for arg in args]
    args = [
        arg.reshape(3, 3, arg.shape[0] // 9, chans) if place in convs else arg
        for place, arg in enumerate(args)
    ]

    scratch = []
    for place, arg in enumerate(args):
        shape = (4, *arg.shape) if place == 1 else arg.shape
        shape = (4, *shape[1:]) if place in convs else shape
        scratch.append(pltpu.VMEM(shape, arg.dtype))
    scratch += [
        pltpu.VMEM((5, tokens, feat), BF16),
        pltpu.VMEM((8, tokens, 4 * feat), BF16),
        pltpu.VMEM((7, tokens, 4 * chans), BF16),
        pltpu.VMEM((4, tokens, 2 * chans), BF16),
        pltpu.VMEM((4, tokens, 2 * chans), F32),
        pltpu.VMEM((6, tokens, 4 * chans), BF16),
        pltpu.VMEM((6, tokens, 4 * chans), BF16),
        pltpu.VMEM((2, tokens, 2 * chans), BF16),
        pltpu.VMEM((4, tokens, 4 * chans), BF16),
        pltpu.VMEM((2, chans // LANES, 2 * tokens, LANES), F32),
        pltpu.VMEM((2, 4, tokens, chans), F32),
        pltpu.SemaphoreType.DMA((17,)),
        pltpu.SemaphoreType.DMA((KINDS,)),
        pltpu.SemaphoreType.DMA((KINDS,)),
    ]
    mid = pl.pallas_call(
        functools.partial(kernel, count),
        out_shape=pltpu.VMEM((2, 2 * tokens, chans), BF16),
        in_specs=[pl.BlockSpec(memory_space=pl.ANY)] * len(args),
        out_specs=pl.BlockSpec(memory_space=pltpu.VMEM),
        scratch_shapes=scratch,
        compiler_params=pltpu.CompilerParams(
            collective_id=0, has_side_effects=True, vmem_limit_bytes=60 * 2**20
        ),
        name="fused_tap",
    )(*args)

    return mid


def solution(mesh):
    return jax.shard_map(
        body,
        mesh=mesh,
        in_specs=(P(("groups", "rows"), None),) * 2 + (P(),) * 15,
        out_specs=P(("groups", "rows"), None, None),
        check_vma=False,
    )
```

```python
import functools

import jax
import jax.numpy as jnp
from jax import lax
from jax.experimental import pallas as pl
from jax.experimental.pallas import tpu as pltpu
from jax.sharding import PartitionSpec as P

GW = 192
BF16 = jnp.bfloat16
F32 = jnp.float32

PIECES = 2
PJ_SIB, PJ_THREE, CO_SIB, CO_ONE, CO_TWO, S_REA, S_IN1, S_MER, S_FAR = range(9)
PJ_ONE = 9
PJ_TWO = PJ_ONE + PIECES
KINDS = PJ_TWO + PIECES
STRIP = 64
LANES = 128


def dot(a, b):
    return jnp.dot(a, b, preferred_element_type=F32)


def put(slab, row, even, odd):
    width, chans = even.shape
    at = lax.broadcasted_iota(jnp.int32, even.shape, 0)
    before = jnp.where(at == 0, 0.0, pltpu.roll(odd, 1, 0)).astype(BF16)
    after = jnp.where(at == width - 1, 0.0, pltpu.roll(even, width - 1, 0)).astype(BF16)
    even, odd = even.astype(BF16), odd.astype(BF16)
    for group, value in enumerate((before - odd, even + odd, even - after, odd - even)):
        slab[row, :, group * chans : (group + 1) * chans] = value


def prepare(weight):
    depth = weight.shape[2]

    def strip(step, carry):
        rows = pl.ds(pl.multiple_of(step * STRIP, STRIP), STRIP)
        for k in range(3):
            outer = 0.5 * (weight[0, k, rows, :].astype(F32) + weight[2, k, rows, :].astype(F32))
            inner = 0.5 * weight[1, k, rows, :].astype(F32)
            weight[1, k, rows, :] = (outer + inner).astype(BF16)
            weight[3, k, rows, :] = (outer - inner).astype(BF16)
        return carry

    lax.fori_loop(0, depth // STRIP, strip, 0)


def kernel(
    count,
    tap_h,
    coarse_h,
    proj_h,
    proj_bh,
    lift_h,
    lift_bh,
    merge_h,
    out_h,
    out_bh,
    fi_h,
    fi_bh,
    fo_h,
    fo_bh,
    si_h,
    si_bh,
    so_h,
    so_bh,
    result,
    tap,
    coarse,
    proj_w,
    proj_b,
    lift_w,
    lift_b,
    merge_w,
    out_w,
    out_b,
    fi_w,
    fi_b,
    fo_w,
    fo_b,
    si_w,
    si_b,
    so_w,
    so_b,
    pj,
    wid,
    rea,
    rea_raw,
    carried,
    in1,
    mer,
    mer_raw,
    in2,
    woven,
    early,
    local_sem,
    send_sem,
    recv_sem,
):
    width = tap.shape[0]
    feat = proj_w.shape[1]
    chans = out_w.shape[1]
    me = lax.axis_index("rows")
    side = lax.rem(me, 2)
    step = 2 * side - 1
    sibling = me - step

    def inside(device):
        return jnp.logical_and(device >= 0, device < count)

    valid = (True, inside(me + step), inside(me + 2 * step), inside(me + 3 * step))
    back_two = inside(me - 2 * step)

    started = []

    def fetch(src, dst):
        copy = pltpu.make_async_copy(src, dst, local_sem.at[len(started)])
        started.append(copy)
        copy.start()
        return [copy]

    def fetch_conv(src, dst):
        sem = local_sem.at[len(started)]
        for k in range(3):
            pltpu.make_async_copy(
                src.at[side * k + (1 - side) * (2 - k)], dst.at[pl.ds(0, 3), k], sem
            ).start()
        landed = dst.at[pl.ds(0, 3)]
        started.append(pltpu.make_async_copy(landed, landed, sem))
        return [started[-1]]

    def done(copies):
        for copy in copies:
            copy.wait()

    tap_in = fetch(tap_h, tap) + fetch(proj_h, proj_w) + fetch(proj_bh, proj_b)
    coarse_in = fetch(coarse_h, coarse.at[0])
    lift_in = fetch(lift_bh, lift_b)
    half = 2 * feat
    lift_sem = local_sem.at[len(started)]
    for m in range(2):
        where = pl.multiple_of((side * m + (1 - side) * (1 - m)) * half, half)
        pltpu.make_async_copy(
            lift_h.at[:, pl.ds(where, half)], lift_w.at[:, pl.ds(m * half, half)], lift_sem
        ).start()
    started.append(pltpu.make_async_copy(lift_w, lift_w, lift_sem))
    lift_in.append(started[-1])

    partners = (
        (me + step, valid[1]),
        (me + 2 * step, valid[2]),
        (me - 2 * step, back_two),
        (me + 3 * step, valid[3]),
    )
    barrier = pltpu.get_barrier_semaphore()
    expected = jnp.int32(1)
    pl.semaphore_signal(
        barrier, inc=1, device_id={"rows": sibling}, device_id_type=pl.DeviceIdType.MESH
    )
    for device, there in partners:

        @pl.when(there)
        def _():
            pl.semaphore_signal(
                barrier, inc=1, device_id={"rows": device}, device_id_type=pl.DeviceIdType.MESH
            )

        expected = expected + there.astype(jnp.int32)

    def remote(src, dst, kind, device):
        return pltpu.make_async_remote_copy(
            src_ref=src,
            dst_ref=dst,
            send_sem=send_sem.at[kind],
            recv_sem=recv_sem.at[kind],
            device_id={"rows": device},
            device_id_type=pl.DeviceIdType.MESH,
        )

    sent = []

    def send(src, dst, kind, device, there=None):
        sent.append((remote(src, dst, kind, device), there))
        if there is None:
            sent[-1][0].start()
        else:
            pl.when(there)(sent[-1][0].start)

    def received(dst, kind, there=None):
        copy = remote(dst, dst, kind, sibling)
        if there is None:
            copy.wait_recv()
        else:
            pl.when(there)(copy.wait_recv)

    done(tap_in)
    merge_in = fetch_conv(merge_h, merge_w)
    out_in = fetch(out_h, out_w) + fetch(out_bh, out_b)
    fi_in = fetch(fi_bh, fi_b) + fetch_conv(fi_h, fi_w)
    fo_in = fetch(fo_bh, fo_b) + fetch_conv(fo_h, fo_w)
    si_in = fetch(si_bh, si_b) + fetch_conv(si_h, si_w)
    so_in = fetch(so_bh, so_b) + fetch_conv(so_h, so_w)
    pj[0] = (dot(tap[...], proj_w[...]) + proj_b[...]).astype(BF16)

    piece = width // PIECES

    def part(slot, k):
        return pj.at[slot, pl.ds(k * piece, piece)]

    pl.semaphore_wait(barrier, expected)
    at_end = jnp.logical_and(back_two, jnp.logical_not(valid[1]))
    to_end = jnp.logical_and(
        jnp.logical_and(back_two, valid[1]), jnp.logical_not(inside(me - 4 * step))
    )
    relays = jnp.logical_and(valid[3], inside(me + 5 * step))
    for k in range(PIECES):
        send(part(0, k), part(1, k), PJ_ONE + k, me + step, valid[1])
    send(pj.at[0], pj.at[4], PJ_SIB, sibling)
    done(coarse_in)
    send(coarse.at[0], coarse.at[3], CO_SIB, sibling)

    def pass_on(k):
        received(part(1, k), PJ_ONE + k, valid[1])
        send(part(1, k), part(2, k), PJ_TWO + k, me + 3 * step, relays)

    def lift(token, slab_token, halves):
        for m in halves:
            both = dot(pj[slab_token], lift_w[:, m * half : (m + 1) * half])
            even = both[:, :feat] + lift_b[...]
            odd = both[:, feat:] + lift_b[...]
            if token > 0:
                even = jnp.where(valid[token], even, 0.0)
                odd = jnp.where(valid[token], odd, 0.0)
            put(wid, 2 * token + m + 1, even, odd)

    def product(slab, weight, row, place, low, high):
        group = slab.shape[2] // 4
        lanes = slice(place * group, (place + 1) * group)
        cells = [slab[row + k, :, lanes] for k in range(low, high)]
        taps = weight[place, low:high].reshape((high - low) * group, chans)
        return dot(jnp.concatenate(cells, axis=1), taps)

    early_taps = {1: 2, 2: 1, 3: 2}

    def ahead(row):
        for place in range(4):
            early[(row - 1) % 2, place] = product(wid, merge_w, row, place, 0, early_taps[row])

    def conv(slab, weight, low, high, base=1):
        rows = high - low
        known = early_taps.get(low, 0) if slab is wid else 0
        products = []
        for place in range(4):
            if known:
                late = product(slab, weight, low, place, known, 3)
                products.append(late + early[(low - 1) % 2, place])
            else:
                products.append(product(slab, weight, low + base - 1, place, 0, 3))
        first, total, last, spread = products
        even = (total + spread) + first
        odd = (total - spread) - last
        return even.reshape(rows, width, chans), odd.reshape(rows, width, chans)

    def keep(row, value):
        return value if row < 2 else jnp.where(valid[row // 2], value, 0.0)

    def merge_rows(low, high):
        even, odd = conv(wid, merge_w, low, high)
        for row in range(low, high):
            e, o = keep(row, even[row - low]), keep(row, odd[row - low])
            if row < 4:
                rea_raw[row, :, :chans] = e.astype(BF16)
                rea_raw[row, :, chans:] = o.astype(BF16)
            put(rea, row + 1, jnp.maximum(e, 0.0), jnp.maximum(o, 0.0))

    def inner_rows(src, weight, bias, dst, low, high, base=1):
        even, odd = conv(src, weight, low, high, base)
        for row in range(low, high):
            e = jnp.maximum(even[row - low] + bias[...], 0.0)
            o = jnp.maximum(odd[row - low] + bias[...], 0.0)
            put(dst, row + 1, keep(row, e), keep(row, o))

    def merged_rows(low, high):
        even, odd = conv(in1, fo_w, low, high)
        for row in range(low, high):
            outer = []
            for parity, value in enumerate((even, odd)):
                lanes = slice(parity * chans, (parity + 1) * chans)
                whole = (
                    value[row - low]
                    + fo_b[...]
                    + rea_raw[row, :, lanes].astype(F32)
                    + carried[row, :, lanes]
                )
                whole = keep(row, whole)
                if row < 2:
                    mer_raw[row, :, lanes] = whole.astype(BF16)
                outer.append(jnp.maximum(whole, 0.0))
            put(mer, row + 2, *outer)

    def carry(row, near, far):
        other = coarse[far].astype(F32)
        if row == 1:
            other = jnp.where(valid[1], other, coarse[near].astype(F32))
        band = 0.75 * coarse[near].astype(F32) + 0.25 * other
        at = lax.broadcasted_iota(jnp.int32, band.shape, 0)
        before = jnp.where(at == 0, band, pltpu.roll(band, 1, 0))
        after = jnp.where(at == width - 1, band, pltpu.roll(band, width - 1, 0))
        for parity, other in enumerate((before, after)):
            spread = (0.75 * band + 0.25 * other).astype(BF16)
            carried[row, :, parity * chans : (parity + 1) * chans] = (
                dot(spread, out_w[...]) + out_b[...]
            )

    def merge_row(row):
        merge_rows(row, row + 1)

    def first_row(row):
        inner_rows(rea, fi_w, fi_b, in1, row, row + 1)

    def merged_row(row):
        merged_rows(row, row + 1)

    def second_row(row):
        inner_rows(mer, si_w, si_b, in2, row, row + 1, 2)

    def final_row(row):
        even, odd = conv(in2, so_w, row, row + 1)
        for parity, value in enumerate((even[0], odd[0])):
            lanes = slice(parity * chans, (parity + 1) * chans)
            united = value + so_b[...] + mer_raw[row, :, lanes].astype(F32)
            for block in range(chans // LANES):
                cells = united[:, block * LANES : (block + 1) * LANES]
                woven[row, block, pl.ds(parity, width, stride=2), :] = cells
        target = side * row + (1 - side) * (1 - row)
        for block in range(chans // LANES):
            lanes = slice(block * LANES, (block + 1) * LANES)
            result[pl.ds(target, 1), :, lanes] = woven[row, block].astype(BF16)[None]

    done(lift_in)
    lift(0, 0, (0, 1))
    send(pj.at[0], pj.at[3], PJ_THREE, me + 3 * step, valid[3])
    done(merge_in)
    prepare(merge_w)
    received(pj.at[4], PJ_SIB)
    lift(-1, 4, (1,))
    for k in range(PIECES):
        send(part(0, k), part(2, k), PJ_TWO + k, me - 2 * step, to_end)
    merge_row(0)
    send(rea.at[1], rea.at[0], S_REA, sibling)
    done(out_in)
    received(coarse.at[3], CO_SIB)
    carry(0, 0, 3)
    done(fi_in)
    prepare(fi_w)
    ahead(1)
    ahead(2)
    pass_on(0)
    done(fo_in)
    prepare(fo_w)
    done(si_in)
    prepare(si_w)
    done(so_in)
    prepare(so_w)
    received(rea.at[0], S_REA)
    pass_on(1)
    for k in range(PIECES):
        send(part(0, k), part(2, k), PJ_TWO + k, me - 2 * step, at_end)
    lift(1, 1, (0, 1))
    merge_row(1)
    merge_row(2)
    first_row(0)
    first_row(1)
    send(in1.at[1], in1.at[0], S_IN1, sibling)
    send(coarse.at[0], coarse.at[1], CO_ONE, me + step, valid[1])
    send(coarse.at[0], coarse.at[2], CO_TWO, me - 2 * step, back_two)
    received(pj.at[3], PJ_THREE, valid[3])
    lift(3, 3, (0,))
    ahead(3)

    for k in range(PIECES):
        received(part(2, k), PJ_TWO + k, valid[2])
    lift(2, 2, (0, 1))
    merge_row(3)
    merge_row(4)
    first_row(2)
    received(in1.at[0], S_IN1)
    merged_row(0)
    merge_row(5)
    first_row(3)
    first_row(4)
    send(mer.at[2], mer.at[1], S_MER, sibling)
    received(coarse.at[1], CO_ONE, valid[1])
    received(coarse.at[2], CO_TWO, valid[2])
    carry(1, 0, 1)
    merged_row(1)
    carry(2, 1, 0)
    send(mer.at[3], mer.at[0], S_FAR, sibling)
    merged_row(2)
    carry(3, 1, 2)
    second_row(1)
    merged_row(3)
    second_row(2)
    received(mer.at[1], S_MER)
    received(mer.at[0], S_FAR)
    second_row(0)
    second_row(-1)
    final_row(1)
    final_row(0)

    for copy, there in sent:
        if there is None:
            copy.wait_send()
        else:
            pl.when(there)(copy.wait_send)


def body(*args):
    count = lax.axis_size("rows")
    tap_two, coarse_path, proj_weight = args[:3]
    tokens, depth = tap_two.shape
    feat, chans = proj_weight.shape[1], coarse_path.shape[1]
    assert tokens == GW and count % 2 == 0
    convs = (6, 9, 11, 13, 15)
    args = [arg.reshape(1, -1) if arg.ndim == 1 else arg for arg in args]
    args = [
        arg.reshape(3, 3, arg.shape[0] // 9, chans) if place in convs else arg
        for place, arg in enumerate(args)
    ]

    scratch = []
    for place, arg in enumerate(args):
        shape = (4, *arg.shape) if place == 1 else arg.shape
        shape = (4, *shape[1:]) if place in convs else shape
        scratch.append(pltpu.VMEM(shape, arg.dtype))
    scratch += [
        pltpu.VMEM((5, tokens, feat), BF16),
        pltpu.VMEM((8, tokens, 4 * feat), BF16),
        pltpu.VMEM((7, tokens, 4 * chans), BF16),
        pltpu.VMEM((4, tokens, 2 * chans), BF16),
        pltpu.VMEM((4, tokens, 2 * chans), F32),
        pltpu.VMEM((6, tokens, 4 * chans), BF16),
        pltpu.VMEM((6, tokens, 4 * chans), BF16),
        pltpu.VMEM((2, tokens, 2 * chans), BF16),
        pltpu.VMEM((4, tokens, 4 * chans), BF16),
        pltpu.VMEM((2, chans // LANES, 2 * tokens, LANES), F32),
        pltpu.VMEM((2, 4, tokens, chans), F32),
        pltpu.SemaphoreType.DMA((17,)),
        pltpu.SemaphoreType.DMA((KINDS,)),
        pltpu.SemaphoreType.DMA((KINDS,)),
    ]
    mid = pl.pallas_call(
        functools.partial(kernel, count),
        out_shape=pltpu.VMEM((2, 2 * tokens, chans), BF16),
        in_specs=[pl.BlockSpec(memory_space=pl.ANY)] * len(args),
        out_specs=pl.BlockSpec(memory_space=pltpu.VMEM),
        scratch_shapes=scratch,
        compiler_params=pltpu.CompilerParams(
            collective_id=0, has_side_effects=True, vmem_limit_bytes=60 * 2**20
        ),
        name="fused_tap",
    )(*args)

    return mid


def solution(mesh):
    return jax.shard_map(
        body,
        mesh=mesh,
        in_specs=(P(("groups", "rows"), None),) * 2 + (P(),) * 15,
        out_specs=P(("groups", "rows"), None, None),
        check_vma=False,
    )
```
